32 devices in a mesh: shard: 8 (over y, x, core), tp: 4 (over z).
Axes of the slice: x: 2, y: 2, z: 4, core: 2. Of those that a mesh axis runs over, the one named last changes fastest.
Arguments:
- weight_gate: bfloat16 [2560, 9728], P('shard', 'tp'), may hold values from -0.15625 to 0.15625
- low_gate: bfloat16 [2560, 32], P('shard'), may hold values from -0.125 to 0.125
- high_gate: bfloat16 [32, 9728], P(None, 'tp'), may hold values from -1 to 1
- weight_up: bfloat16 [2560, 9728], P('shard', 'tp'), may hold values from -0.15625 to 0.15625
- low_up: bfloat16 [2560, 32], P('shard'), may hold values from -0.125 to 0.125
- high_up: bfloat16 [32, 9728], P(None, 'tp'), may hold values from -1 to 1
- norm_gain: float32 [2560], P('shard'), may hold values from 0.25 to 1.75
Outputs:
- ready_gate: bfloat16 [2560, 9728], P(None, 'tp')
- ready_up: bfloat16 [2560, 9728], P(None, 'tp')
- factor_gate: float32 [9728], P('tp')
- factor_up: float32 [9728], P('tp')
The draws below stay inside these ranges and needn't reach their ends.
All inputs are finite; a program needn't handle non-finite values.
Results may differ from the reference program's by a relative error of at most 0.001.
Values may be sent and summed in bfloat16 or wider, within the bound.
A program may use at most 128 MiB of HBM per device.

```python
import jax
import jax.numpy as jnp
from jax import lax

D_MODEL = 2560
D_INNER = 9728
RANK = 32


def spiked(result, rng, source, target, shards_of, factor):
    owner, partner = [(jnp.arange(result.shape[dim]) // (result.shape[dim] // shards_of)).reshape([-1 if axis == dim else 1 for axis in range(result.ndim)]) for dim in (source, target)]
    chosen = jax.random.permutation(rng, shards_of)[partner]
    strong = (owner == chosen) | (owner == (partner + shards_of // 2) % shards_of)
    return jnp.where(strong, factor * result, result)


def block_scale(stream_key, dims, split, low, largest):
    loudness, own = 1.0, jax.random.fold_in(stream_key, 6)
    for position, shards_of in split:
        draws = jnp.exp(jax.random.uniform(jax.random.fold_in(own, position), (shards_of,), jnp.float32, low / len(split), largest / len(split)))
        loudness = loudness * jnp.repeat(draws, dims[position] // shards_of).reshape([-1 if axis == position else 1 for axis in range(len(dims))])
    return loudness


def scatter_about(rng, shape, scale, most, shards=(), dtype=jnp.bfloat16):
    drawn = jax.random.normal(rng, shape, jnp.float32) * scale
    if len(shards) > 0:
        drawn = block_scale(rng, shape, shards, -0.22, 0.18) * drawn
    return jnp.clip(drawn, min=-most, max=most).astype(dtype)


def bell_draw_with(key, shape, scale, bound, shards, heavy, kind=jnp.bfloat16):
    array = scale * jax.random.normal(key, shape, jnp.float32)
    if shards:
        array = array * block_scale(key, shape, shards, -0.22, 0.18)
    return jnp.clip(spiked(array, jax.random.fold_in(key, 3), *heavy), -bound, bound).astype(kind)


def setup_inputs(seed: int = 0) -> dict:
    streams_of = jax.random.split(jax.random.key(seed), 8)
    return {
        "weight_gate": bell_draw_with(streams_of[0], (D_MODEL, D_INNER), D_MODEL ** -0.5, 0.15625, ((0, 8), (1, 4)), (0, 1, 8, 2.0)),
        "low_gate": scatter_about(streams_of[1], (D_MODEL, RANK), D_MODEL ** -0.5, 0.125, ((0, 8),)),
        "high_gate": scatter_about(streams_of[2], (RANK, D_INNER), RANK ** -0.5, 1.0, ((1, 4),)),
        "weight_up": bell_draw_with(streams_of[3], (D_MODEL, D_INNER), D_MODEL ** -0.5, 0.15625, ((0, 8), (1, 4)), (0, 1, 8, 2.0)),
        "low_up": scatter_about(streams_of[4], (D_MODEL, RANK), D_MODEL ** -0.5, 0.125, ((0, 8),)),
        "high_up": scatter_about(streams_of[5], (RANK, D_INNER), RANK ** -0.5, 1.0, ((1, 4),)),
        "norm_gain": jnp.clip(1.0 + 0.15 * jax.random.normal(streams_of[6], (D_MODEL,), jnp.float32), 0.25, 1.75),
    }


mix_rate = 2.0

def reference(weight_gate, low_gate, high_gate, weight_up, low_up, high_up, norm_gain):
    latest_gate = weight_gate.astype(jnp.float32) + mix_rate * jnp.dot(low_gate, high_gate, preferred_element_type=jnp.float32)
    latest_up = weight_up.astype(jnp.float32) + mix_rate * jnp.dot(low_up, high_up, preferred_element_type=jnp.float32)
    latest_gained_gate = latest_gate * norm_gain[:, None]
    latest_gained_up = latest_up * norm_gain[:, None]
    factor_gate = jnp.sqrt(lax.optimization_barrier(jnp.sum(latest_gained_gate * latest_gained_gate, axis=0)))
    ready_gate = (latest_gained_gate / factor_gate).astype(jnp.bfloat16)
    factor_up = jnp.sqrt(lax.optimization_barrier(jnp.sum(latest_gained_up * latest_gained_up, axis=0)))
    ready_up = (latest_gained_up / factor_up).astype(jnp.bfloat16)
    return (ready_gate, ready_up, factor_gate, factor_up)
```

```python
import functools
import math

import jax
import jax.numpy as jnp
from jax import lax
from jax.experimental import pallas as pl
from jax.experimental.pallas import tpu as pltpu
from jax.sharding import PartitionSpec as P

mix_rate = 2.0
AXIS = "shard"


def local(weight_gate, low_gate, high_gate, weight_up, low_up, high_up, norm_gain):
    latest_gate = weight_gate.astype(jnp.float32) + mix_rate * jnp.dot(
        low_gate, high_gate, preferred_element_type=jnp.float32
    )
    latest_up = weight_up.astype(jnp.float32) + mix_rate * jnp.dot(
        low_up, high_up, preferred_element_type=jnp.float32
    )
    latest_gained_gate = latest_gate * norm_gain[:, None]
    latest_gained_up = latest_up * norm_gain[:, None]
    total_gate, total_up = lax.psum(
        (
            jnp.sum(latest_gained_gate * latest_gained_gate, axis=0),
            jnp.sum(latest_gained_up * latest_gained_up, axis=0),
        ),
        AXIS,
    )
    factor_gate = jnp.sqrt(total_gate)
    factor_up = jnp.sqrt(total_up)
    narrow_gate = (latest_gained_gate / factor_gate).astype(jnp.bfloat16)
    narrow_up = (latest_gained_up / factor_up).astype(jnp.bfloat16)
    ready_gate = lax.all_gather(narrow_gate, AXIS, axis=0, tiled=True)
    ready_up = lax.all_gather(narrow_up, AXIS, axis=0, tiled=True)
    return (ready_gate, ready_up, factor_gate, factor_up)


def gather_kernel(
    n, chunks, wg_hbm, wu_hbm, lg, lu, hg, hu, gain,
    out_g, out_u, fac,
    w_v, g_v, col_v, sums, rf_v, w_sem, ssum, rsum, send, recv,
):
    rows, cols = wg_hbm.shape
    step = rows // chunks
    me = lax.axis_index(AXIS)
    core = lax.rem(me, 2)
    x = lax.rem(me // 2, 2)
    y = me // 4
    sib = me + 1 - 2 * core
    to_x = me + 2 - 4 * x
    to_y = me + 4 - 8 * y
    diag = to_x + 4 - 8 * y

    barrier = pltpu.get_barrier_semaphore()
    for d in range(1, n):
        pl.semaphore_signal(barrier, inc=1, device_id={AXIS: lax.rem(me + d, n)})

    loads = [
        pltpu.make_async_copy(w, w_v.at[a], w_sem.at[a])
        for a, w in enumerate((wg_hbm, wu_hbm))
    ]
    for c in loads:
        c.start()

    wide = jnp.broadcast_to(gain[...], (128, gain.shape[1]))
    col_v[...] = wide.T
    lows, highs, outs = (lg, lu), (hg, hu), (out_g, out_u)
    for a in range(2):
        loads[a].wait()
        acc = jnp.zeros((8, cols), jnp.float32)
        for k in range(chunks):
            r = pl.ds(k * step, step)
            prod = jnp.dot(lows[a][r, :], highs[a][...], preferred_element_type=jnp.float32)
            new = w_v[a, r, :].astype(jnp.float32) + mix_rate * prod
            new = new * col_v[r, 0:1]
            g_v[a, r, :] = new
            acc = acc + jnp.sum((new * new).reshape(step // 8, 8, cols), axis=0)
        sums[me, :, a * cols:(a + 1) * cols] = jnp.sum(acc, axis=0, keepdims=True)

    pl.semaphore_wait(barrier, n - 1)
    shares = []
    for d in range(1, n):
        shares.append(pltpu.make_async_remote_copy(
            src_ref=sums.at[me], dst_ref=sums.at[me],
            send_sem=ssum.at[d], recv_sem=rsum.at[d],
            device_id={AXIS: lax.rem(me + d, n)}))
        shares[-1].start()
    for c in shares:
        c.wait_recv()
    total = sums[0]
    for d in range(1, n):
        total = total + sums[d]
    factor = jnp.sqrt(total)
    fac[...] = factor
    rf_v[...] = 1.0 / factor

    def move(slot, a, k, owner, target):
        r = pl.ds(pl.multiple_of(owner * rows + k * step, 16), step)
        part = outs[a].at[r, :]
        return pltpu.make_async_remote_copy(
            src_ref=part, dst_ref=part,
            send_sem=send.at[slot, a * chunks + k], recv_sem=recv.at[slot, a * chunks + k],
            device_id={AXIS: target})

    started = []

    def go(*args):
        c = move(*args)
        c.start()
        started.append(c)

    every = [(a, k) for a in range(2) for k in range(chunks)]

    def send_own(a, k):
        go(0, a, k, me, to_x)
        go(1, a, k, me, to_y)
        go(2, a, k, me, sib)

    for i, (a, k) in enumerate(every):
        new = g_v[a, k * step:(k + 1) * step, :] * rf_v[:, a * cols:(a + 1) * cols]
        r = pl.ds(pl.multiple_of(me * rows + k * step, 16), step)
        outs[a][r, :] = new.astype(jnp.bfloat16)
        if i:
            send_own(*every[i - 1])
    send_own(*every[-1])

    for a, k in every:
        move(0, a, k, to_x, to_x).wait_recv()
        if k % 2 == 0:
            go(5, a, k, to_x, to_y)
        go(3, a, k, to_x, sib)
        move(1, a, k, to_y, to_y).wait_recv()
        if k % 2 == 1:
            go(5, a, k, to_y, to_x)
        go(4, a, k, to_y, sib)
    for a, k in every:
        move(5, a, k, diag, to_x).wait_recv()
        go(6, a, k, diag, sib)
    flip = 1 - 2 * core
    for a, k in every:
        move(2, a, k, sib, sib).wait_recv()
        move(3, a, k, to_x + flip, sib).wait_recv()
        move(4, a, k, to_y + flip, sib).wait_recv()
        move(6, a, k, diag + flip, sib).wait_recv()
    for c in started:
        c.wait_send()
    for c in shares:
        c.wait_send()


def write_kernel(parts, a_v, b_v, a_hbm, b_hbm, sem):
    step = a_v.shape[0] // parts
    copies = []
    for i, (src, dst) in enumerate(((a_v, a_hbm), (b_v, b_hbm))):
        for k in range(parts):
            r = pl.ds(k * step, step)
            copies.append(pltpu.make_async_copy(src.at[r, :], dst.at[r, :], sem.at[i, k]))
    for c in copies:
        c.start()
    for c in copies:
        c.wait()


def paired(n, weight_gate, low_gate, high_gate, weight_up, low_up, high_up, norm_gain):
    rows, cols = weight_gate.shape
    chunks = 4
    full = (n * rows, cols)
    vmem = pl.BlockSpec(memory_space=pltpu.VMEM)
    hbm = pl.BlockSpec(memory_space=pl.ANY)
    padded = -(-rows // 128) * 128
    gain = jnp.pad(norm_gain, (0, padded - rows)).reshape(1, padded)
    gate, up, fac = pl.pallas_call(
        functools.partial(gather_kernel, n, chunks),
        out_shape=(
            pltpu.VMEM(full, jnp.bfloat16),
            pltpu.VMEM(full, jnp.bfloat16),
            jax.ShapeDtypeStruct((1, 2 * cols), jnp.float32),
        ),
        in_specs=[hbm, hbm] + [vmem] * 5,
        out_specs=(vmem, vmem, vmem),
        scratch_shapes=[
            pltpu.VMEM((2, rows, cols), jnp.bfloat16),
            pltpu.VMEM((2, rows, cols), jnp.float32),
            pltpu.VMEM((padded, 128), jnp.float32),
            pltpu.VMEM((n, 1, 2 * cols), jnp.float32),
            pltpu.VMEM((1, 2 * cols), jnp.float32),
            pltpu.SemaphoreType.DMA((2,)),
            pltpu.SemaphoreType.DMA((n,)),
            pltpu.SemaphoreType.DMA((n,)),
            pltpu.SemaphoreType.DMA((7, 2 * chunks)),
            pltpu.SemaphoreType.DMA((7, 2 * chunks)),
        ],
        compiler_params=pltpu.CompilerParams(
            collective_id=0, has_side_effects=True, vmem_limit_bytes=24 * 2**20
        ),
        name="merge_gather",
    )(weight_gate, weight_up, low_gate, low_up, high_gate, high_up, gain)
    parts = 8
    ready_gate, ready_up = pl.pallas_call(
        functools.partial(write_kernel, parts),
        out_shape=(jax.ShapeDtypeStruct(full, jnp.bfloat16),) * 2,
        in_specs=[vmem, vmem],
        out_specs=(hbm, hbm),
        scratch_shapes=[pltpu.SemaphoreType.DMA((2, parts))],
        compiler_params=pltpu.CompilerParams(vmem_limit_bytes=2**20),
        name="write_out",
    )(gate, up)
    return ready_gate, ready_up, fac[0, :cols], fac[0, cols:]


def solution(mesh):
    in_specs = (
        P("shard", "tp"),
        P("shard", None),
        P(None, "tp"),
        P("shard", "tp"),
        P("shard", None),
        P(None, "tp"),
        P("shard"),
    )
    out_specs = (P(None, "tp"), P(None, "tp"), P("tp"), P("tp"))
    n = mesh.shape[AXIS]
    side = math.isqrt(n // 2)
    body = functools.partial(paired, n) if side == 2 and 2 * side * side == n else local
    return jax.shard_map(body, mesh=mesh, in_specs=in_specs, out_specs=out_specs, check_vma=False)
```

```python
import functools
import math

import jax
import jax.numpy as jnp
from jax import lax
from jax.experimental import pallas as pl
from jax.experimental.pallas import tpu as pltpu
from jax.sharding import PartitionSpec as P

mix_rate = 2.0
AXIS = "shard"


def local(weight_gate, low_gate, high_gate, weight_up, low_up, high_up, norm_gain):
    latest_gate = weight_gate.astype(jnp.float32) + mix_rate * jnp.dot(
        low_gate, high_gate, preferred_element_type=jnp.float32
    )
    latest_up = weight_up.astype(jnp.float32) + mix_rate * jnp.dot(
        low_up, high_up, preferred_element_type=jnp.float32
    )
    latest_gained_gate = latest_gate * norm_gain[:, None]
    latest_gained_up = latest_up * norm_gain[:, None]
    total_gate, total_up = lax.psum(
        (
            jnp.sum(latest_gained_gate * latest_gained_gate, axis=0),
            jnp.sum(latest_gained_up * latest_gained_up, axis=0),
        ),
        AXIS,
    )
    factor_gate = jnp.sqrt(total_gate)
    factor_up = jnp.sqrt(total_up)
    narrow_gate = (latest_gained_gate / factor_gate).astype(jnp.bfloat16)
    narrow_up = (latest_gained_up / factor_up).astype(jnp.bfloat16)
    ready_gate = lax.all_gather(narrow_gate, AXIS, axis=0, tiled=True)
    ready_up = lax.all_gather(narrow_up, AXIS, axis=0, tiled=True)
    return (ready_gate, ready_up, factor_gate, factor_up)


def gather_kernel(
    n, chunks, wg_hbm, wu_hbm, lg_hbm, lu_hbm, hg_hbm, hu_hbm, gain_hbm,
    out_g, out_u, fac,
    w_v, l_v, h_v, gain_v, low_v, g_v, col_v, sums, rf_v,
    in_sem, ssum, rsum, send, recv,
):
    rows, cols = wg_hbm.shape
    step = rows // chunks
    me = lax.axis_index(AXIS)
    core = lax.rem(me, 2)
    x = lax.rem(me // 2, 2)
    y = me // 4
    sib = me + 1 - 2 * core
    to_x = me + 2 - 4 * x
    to_y = me + 4 - 8 * y
    diag = to_x + 4 - 8 * y

    barrier = pltpu.get_barrier_semaphore()
    for d in range(1, n):
        pl.semaphore_signal(barrier, inc=1, device_id={AXIS: lax.rem(me + d, n)})

    gain_load = pltpu.make_async_copy(gain_hbm, gain_v, in_sem.at[6])
    low_loads, high_loads, loads = (
        [
            pltpu.make_async_copy(src, dst.at[a], in_sem.at[3 * a + i])
            for a, src in enumerate(pair)
        ]
        for i, (pair, dst) in enumerate((
            ((lg_hbm, lu_hbm), l_v), ((hg_hbm, hu_hbm), h_v), ((wg_hbm, wu_hbm), w_v)
        ))
    )
    gain_load.start()
    for a in range(2):
        for c in (low_loads[a], high_loads[a], loads[a]):
            c.start()

    gain_load.wait()
    col_v[...] = jnp.broadcast_to(gain_v[...], (128, rows)).T
    outs = (out_g, out_u)
    for a in range(2):
        low_loads[a].wait()
        low_v[a] = (mix_rate * l_v[a].astype(jnp.float32)).T.astype(jnp.bfloat16)
        high_loads[a].wait()
        loads[a].wait()
        acc = jnp.zeros((8, cols), jnp.float32)
        for k in range(chunks):
            r = pl.ds(k * step, step)
            prod = jnp.dot(low_v[a, r, :], h_v[a], preferred_element_type=jnp.float32)
            new = (w_v[a, r, :].astype(jnp.float32) + prod) * col_v[r, 0:1]
            g_v[a, r, :] = new
            acc = acc + jnp.sum((new * new).reshape(step // 8, 8, cols), axis=0)
        sums[me, :, a * cols:(a + 1) * cols] = jnp.sum(acc, axis=0, keepdims=True)

    pl.semaphore_wait(barrier, n - 1)
    shares = []
    for d in range(1, n):
        shares.append(pltpu.make_async_remote_copy(
            src_ref=sums.at[me], dst_ref=sums.at[me],
            send_sem=ssum.at[d], recv_sem=rsum.at[d],
            device_id={AXIS: lax.rem(me + d, n)}))
        shares[-1].start()
    for c in shares:
        c.wait_recv()
    total = sums[0]
    for d in range(1, n):
        total = total + sums[d]
    factor = jnp.sqrt(total)
    fac[...] = factor
    rf_v[...] = 1.0 / factor

    def move(slot, a, k, owner, target):
        r = pl.ds(pl.multiple_of(owner * rows + k * step, 16), step)
        part = outs[a].at[r, :]
        return pltpu.make_async_remote_copy(
            src_ref=part, dst_ref=part,
            send_sem=send.at[slot, a * chunks + k], recv_sem=recv.at[slot, a * chunks + k],
            device_id={AXIS: target})

    started = []

    def go(*args):
        c = move(*args)
        c.start()
        started.append(c)

    every = [(a, k) for a in range(2) for k in range(chunks)]

    def send_own(a, k):
        go(0, a, k, me, to_x)
        go(1, a, k, me, to_y)
        go(2, a, k, me, sib)

    for i, (a, k) in enumerate(every):
        new = g_v[a, k * step:(k + 1) * step, :] * rf_v[:, a * cols:(a + 1) * cols]
        r = pl.ds(pl.multiple_of(me * rows + k * step, 16), step)
        outs[a][r, :] = new.astype(jnp.bfloat16)
        if i:
            send_own(*every[i - 1])
    send_own(*every[-1])

    for a, k in every:
        move(0, a, k, to_x, to_x).wait_recv()
        if k % 2 == 0:
            go(5, a, k, to_x, to_y)
        go(3, a, k, to_x, sib)
        move(1, a, k, to_y, to_y).wait_recv()
        if k % 2 == 1:
            go(5, a, k, to_y, to_x)
        go(4, a, k, to_y, sib)
    for a, k in every:
        move(5, a, k, diag, to_x).wait_recv()
        go(6, a, k, diag, sib)
    flip = 1 - 2 * core
    for a, k in every:
        move(2, a, k, sib, sib).wait_recv()
        move(3, a, k, to_x + flip, sib).wait_recv()
        move(4, a, k, to_y + flip, sib).wait_recv()
        move(6, a, k, diag + flip, sib).wait_recv()
    for c in started:
        c.wait_send()
    for c in shares:
        c.wait_send()


def write_kernel(parts, a_v, b_v, a_hbm, b_hbm, sem):
    step = a_v.shape[0] // parts
    copies = []
    for i, (src, dst) in enumerate(((a_v, a_hbm), (b_v, b_hbm))):
        for k in range(parts):
            r = pl.ds(k * step, step)
            copies.append(pltpu.make_async_copy(src.at[r, :], dst.at[r, :], sem.at[i, k]))
    for c in copies:
        c.start()
    for c in copies:
        c.wait()


def paired(n, weight_gate, low_gate, high_gate, weight_up, low_up, high_up, norm_gain):
    rows, cols = weight_gate.shape
    chunks = 4
    full = (n * rows, cols)
    vmem = pl.BlockSpec(memory_space=pltpu.VMEM)
    hbm = pl.BlockSpec(memory_space=pl.ANY)
    gain = norm_gain.reshape(1, rows)
    space = pl.BlockSpec(memory_space=pltpu.HBM)
    rank = high_gate.shape[0]
    grant = 65472 * 2**10 - (4 * full[0] * cols + 8 * cols) // 2**10 * 2**10 - 24 * 2**10
    gate, up, fac = pl.pallas_call(
        functools.partial(gather_kernel, n, chunks),
        out_shape=(
            pltpu.VMEM(full, jnp.bfloat16),
            pltpu.VMEM(full, jnp.bfloat16),
            jax.ShapeDtypeStruct((1, 2 * cols), jnp.float32),
        ),
        in_specs=[space] * 7,
        out_specs=(vmem, vmem, vmem),
        scratch_shapes=[
            pltpu.VMEM((2, rows, cols), jnp.bfloat16),
            pltpu.VMEM((2, rank, rows), jnp.bfloat16),
            pltpu.VMEM((2, rank, cols), jnp.bfloat16),
            pltpu.VMEM((1, rows), jnp.float32),
            pltpu.VMEM((2, rows, rank), jnp.bfloat16),
            pltpu.VMEM((2, rows, cols), jnp.float32),
            pltpu.VMEM((rows, 128), jnp.float32),
            pltpu.VMEM((n, 1, 2 * cols), jnp.float32),
            pltpu.VMEM((1, 2 * cols), jnp.float32),
            pltpu.SemaphoreType.DMA((7,)),
            pltpu.SemaphoreType.DMA((n,)),
            pltpu.SemaphoreType.DMA((n,)),
            pltpu.SemaphoreType.DMA((7, 2 * chunks)),
            pltpu.SemaphoreType.DMA((7, 2 * chunks)),
        ],
        compiler_params=pltpu.CompilerParams(
            collective_id=0, has_side_effects=True, vmem_limit_bytes=grant
        ),
        name="merge_gather",
    )(weight_gate, weight_up, low_gate.T, low_up.T, high_gate, high_up, gain)
    parts = 8
    ready_gate, ready_up = pl.pallas_call(
        functools.partial(write_kernel, parts),
        out_shape=(jax.ShapeDtypeStruct(full, jnp.bfloat16),) * 2,
        in_specs=[vmem, vmem],
        out_specs=(hbm, hbm),
        scratch_shapes=[pltpu.SemaphoreType.DMA((2, parts))],
        compiler_params=pltpu.CompilerParams(vmem_limit_bytes=2**20),
        name="write_out",
    )(gate, up)
    return ready_gate, ready_up, fac[0, :cols], fac[0, cols:]


def solution(mesh):
    in_specs = (
        P("shard", "tp"),
        P("shard", None),
        P(None, "tp"),
        P("shard", "tp"),
        P("shard", None),
        P(None, "tp"),
        P("shard"),
    )
    out_specs = (P(None, "tp"), P(None, "tp"), P("tp"), P("tp"))
    n = mesh.shape[AXIS]
    side = math.isqrt(n // 2)
    body = functools.partial(paired, n) if side == 2 and 2 * side * side == n else local
    return jax.shard_map(body, mesh=mesh, in_specs=in_specs, out_specs=out_specs, check_vma=False)
```

```python
import functools
import math

import jax
import jax.numpy as jnp
from jax import lax
from jax.experimental import pallas as pl
from jax.experimental.pallas import tpu as pltpu
from jax.sharding import PartitionSpec as P

mix_rate = 2.0
AXIS = "shard"


def local(weight_gate, low_gate, high_gate, weight_up, low_up, high_up, norm_gain):
    latest_gate = weight_gate.astype(jnp.float32) + mix_rate * jnp.dot(
        low_gate, high_gate, preferred_element_type=jnp.float32
    )
    latest_up = weight_up.astype(jnp.float32) + mix_rate * jnp.dot(
        low_up, high_up, preferred_element_type=jnp.float32
    )
    latest_gained_gate = latest_gate * norm_gain[:, None]
    latest_gained_up = latest_up * norm_gain[:, None]
    total_gate, total_up = lax.psum(
        (
            jnp.sum(latest_gained_gate * latest_gained_gate, axis=0),
            jnp.sum(latest_gained_up * latest_gained_up, axis=0),
        ),
        AXIS,
    )
    factor_gate = jnp.sqrt(total_gate)
    factor_up = jnp.sqrt(total_up)
    narrow_gate = (latest_gained_gate / factor_gate).astype(jnp.bfloat16)
    narrow_up = (latest_gained_up / factor_up).astype(jnp.bfloat16)
    ready_gate = lax.all_gather(narrow_gate, AXIS, axis=0, tiled=True)
    ready_up = lax.all_gather(narrow_up, AXIS, axis=0, tiled=True)
    return (ready_gate, ready_up, factor_gate, factor_up)


def gather_kernel(
    n, chunks, raw, wg_hbm, wu_hbm, lg_hbm, lu_hbm, hg_hbm, hu_hbm, gain_hbm,
    out_g, out_u, fac,
    w_v, l_v, h_v, gain_v, low_v, g_v, col_v, sums, rf_v, far_low,
    in_sem, ssum, rsum, slow, rlow, send, recv,
):
    rows, cols = wg_hbm.shape
    step = rows // chunks
    me = lax.axis_index(AXIS)
    core = lax.rem(me, 2)
    x = lax.rem(me // 2, 2)
    y = me // 4
    sib = me + 1 - 2 * core
    to_x = me + 2 - 4 * x
    to_y = me + 4 - 8 * y
    diag = to_x + 4 - 8 * y

    barrier = pltpu.get_barrier_semaphore()
    for d in range(1, n):
        pl.semaphore_signal(barrier, inc=1, device_id={AXIS: lax.rem(me + d, n)})

    gain_load = pltpu.make_async_copy(gain_hbm, gain_v, in_sem.at[6])
    low_loads, high_loads, loads = (
        [
            pltpu.make_async_copy(src, dst.at[a], in_sem.at[3 * a + i])
            for a, src in enumerate(pair)
        ]
        for i, (pair, dst) in enumerate((
            ((lg_hbm, lu_hbm), l_v), ((hg_hbm, hu_hbm), h_v), ((wg_hbm, wu_hbm), w_v)
        ))
    )
    gain_load.start()
    for a in range(2):
        for c in (low_loads[a], high_loads[a], loads[a]):
            c.start()

    early = raw * step
    outs = (out_g, out_u)
    every = [(a, k) for a in range(2) for k in range(chunks)]
    started = {}

    def move(slot, a, k, owner, target, base=None):
        r = pl.ds(pl.multiple_of(owner * rows + k * step, 16), step)
        part = outs[a].at[r, :]
        return pltpu.make_async_remote_copy(
            src_ref=part if base is None else base.at[k * step:(k + 1) * step, :],
            dst_ref=part,
            send_sem=send.at[slot, a * chunks + k], recv_sem=recv.at[slot, a * chunks + k],
            device_id={AXIS: target})

    def go(*args):
        started[args[:3]] = move(*args)
        started[args[:3]].start()

    def send_own(a, k):
        go(0, a, k, me, to_x)
        go(1, a, k, me, to_y)
        go(2, a, k, me, sib)

    def send_raw(a, k):
        go(0, a, k, me, to_x, wg_hbm)
        go(1, a, k, me, to_y, wg_hbm)
        go(2, a, k, me, sib, wg_hbm)

    pl.semaphore_wait(barrier, n - 1)
    send_raw(0, 0)

    gain_load.wait()
    col_v[...] = jnp.broadcast_to(gain_v[...], (128, rows)).T
    for a in range(2):
        low_loads[a].wait()
        low_v[a] = (mix_rate * l_v[a].astype(jnp.float32)).T.astype(jnp.bfloat16)
        high_loads[a].wait()
        loads[a].wait()
        acc = jnp.zeros((8, cols), jnp.float32)
        for k in range(chunks):
            r = pl.ds(k * step, step)
            prod = jnp.dot(low_v[a, r, :], h_v[a], preferred_element_type=jnp.float32)
            new = (w_v[a, r, :].astype(jnp.float32) + prod) * col_v[r, 0:1]
            g_v[a, r, :] = new
            acc = acc + jnp.sum((new * new).reshape(step // 8, 8, cols), axis=0)
        sums[me, :, a * cols:(a + 1) * cols] = jnp.sum(acc, axis=0, keepdims=True)

    sums[me, :, 2 * cols:] = gain_v[:, :early]
    shares = []
    for d in range(1, n):
        shares.append(pltpu.make_async_remote_copy(
            src_ref=sums.at[me], dst_ref=sums.at[me],
            send_sem=ssum.at[d], recv_sem=rsum.at[d],
            device_id={AXIS: lax.rem(me + d, n)}))
        shares[-1].start()
    lows = []
    for d in range(1, n):
        lows.append(pltpu.make_async_remote_copy(
            src_ref=l_v.at[0, :, :early], dst_ref=far_low.at[me],
            send_sem=slow.at[d], recv_sem=rlow.at[d],
            device_id={AXIS: lax.rem(me + d, n)}))
        lows[-1].start()
    for k in range(1, raw):
        send_raw(0, k)
    for c in shares:
        c.wait_recv()
    total = sums[0, :, :2 * cols]
    for d in range(1, n):
        total = total + sums[d, :, :2 * cols]
    factor = jnp.sqrt(total)
    fac[...] = factor
    rf_v[...] = 1.0 / factor

    for i, (a, k) in enumerate(every):
        new = g_v[a, k * step:(k + 1) * step, :] * rf_v[:, a * cols:(a + 1) * cols]
        r = pl.ds(pl.multiple_of(me * rows + k * step, 16), step)
        outs[a][r, :] = new.astype(jnp.bfloat16)
        if i > raw:
            send_own(*every[i - 1])
    send_own(*every[-1])

    for i, (a, k) in enumerate(every):
        move(0, a, k, to_x, to_x).wait_recv()
        if i % 2 == 0:
            go(5, a, k, to_x, to_y)
        go(3, a, k, to_x, sib)
        move(1, a, k, to_y, to_y).wait_recv()
        if i % 2 == 1:
            go(5, a, k, to_y, to_x)
        go(4, a, k, to_y, sib)

    flip = 1 - 2 * core

    def from_sib(a, k):
        move(2, a, k, sib, sib).wait_recv()
        move(3, a, k, to_x + flip, sib).wait_recv()
        move(4, a, k, to_y + flip, sib).wait_recv()
        move(6, a, k, diag + flip, sib).wait_recv()

    def finish_raw():
        for a, k in every[:raw]:
            from_sib(a, k)
            for slot in (3, 4, 5, 6):
                started.pop((slot, a, k)).wait_send()
        for c in lows:
            c.wait_recv()

        @pl.loop(1, n)
        def _(d):
            owner = lax.rem(me + d, n)
            low = (mix_rate * far_low[owner].astype(jnp.float32)).T.astype(jnp.bfloat16)
            col = jnp.broadcast_to(sums[owner, :, 2 * cols:], (128, early)).T[:, 0:1]
            r = pl.ds(pl.multiple_of(owner * rows, 16), early)
            prod = jnp.dot(low, h_v[0], preferred_element_type=jnp.float32)
            new = (out_g[r, :].astype(jnp.float32) + prod) * col
            out_g[r, :] = (new * rf_v[:, :cols]).astype(jnp.bfloat16)

    for i, (a, k) in enumerate(every):
        if i == 3 * raw:
            finish_raw()
        move(5, a, k, diag, to_x).wait_recv()
        go(6, a, k, diag, sib)
    for a, k in every[raw:]:
        from_sib(a, k)
    for c in started.values():
        c.wait_send()
    for c in shares + lows:
        c.wait_send()


def write_kernel(parts, a_v, b_v, a_hbm, b_hbm, sem):
    step = a_v.shape[0] // parts
    copies = []
    for i, (src, dst) in enumerate(((a_v, a_hbm), (b_v, b_hbm))):
        for k in range(parts):
            r = pl.ds(k * step, step)
            copies.append(pltpu.make_async_copy(src.at[r, :], dst.at[r, :], sem.at[i, k]))
    for c in copies:
        c.start()
    for c in copies:
        c.wait()


def paired(n, weight_gate, low_gate, high_gate, weight_up, low_up, high_up, norm_gain):
    rows, cols = weight_gate.shape
    chunks, raw = 5, 2
    early = raw * rows // chunks
    full = (n * rows, cols)
    vmem = pl.BlockSpec(memory_space=pltpu.VMEM)
    hbm = pl.BlockSpec(memory_space=pl.ANY)
    gain = norm_gain.reshape(1, rows)
    space = pl.BlockSpec(memory_space=pltpu.HBM)
    rank = high_gate.shape[0]
    grant = 65472 * 2**10 - (4 * full[0] * cols + 8 * cols) // 2**10 * 2**10 - 24 * 2**10
    gate, up, fac = pl.pallas_call(
        functools.partial(gather_kernel, n, chunks, raw),
        out_shape=(
            pltpu.VMEM(full, jnp.bfloat16),
            pltpu.VMEM(full, jnp.bfloat16),
            jax.ShapeDtypeStruct((1, 2 * cols), jnp.float32),
        ),
        in_specs=[space] * 7,
        out_specs=(vmem, vmem, vmem),
        scratch_shapes=[
            pltpu.VMEM((2, rows, cols), jnp.bfloat16),
            pltpu.VMEM((2, rank, rows), jnp.bfloat16),
            pltpu.VMEM((2, rank, cols), jnp.bfloat16),
            pltpu.VMEM((1, rows), jnp.float32),
            pltpu.VMEM((2, rows, rank), jnp.bfloat16),
            pltpu.VMEM((2, rows, cols), jnp.float32),
            pltpu.VMEM((rows, 128), jnp.float32),
            pltpu.VMEM((n, 1, 2 * cols + early), jnp.float32),
            pltpu.VMEM((1, 2 * cols), jnp.float32),
            pltpu.VMEM((n, rank, early), jnp.bfloat16),
            pltpu.SemaphoreType.DMA((7,)),
            pltpu.SemaphoreType.DMA((n,)),
            pltpu.SemaphoreType.DMA((n,)),
            pltpu.SemaphoreType.DMA((n,)),
            pltpu.SemaphoreType.DMA((n,)),
            pltpu.SemaphoreType.DMA((7, 2 * chunks)),
            pltpu.SemaphoreType.DMA((7, 2 * chunks)),
        ],
        compiler_params=pltpu.CompilerParams(
            collective_id=0, has_side_effects=True, vmem_limit_bytes=grant
        ),
        name="merge_gather",
    )(weight_gate, weight_up, low_gate.T, low_up.T, high_gate, high_up, gain)
    parts = 8
    ready_gate, ready_up = pl.pallas_call(
        functools.partial(write_kernel, parts),
        out_shape=(jax.ShapeDtypeStruct(full, jnp.bfloat16),) * 2,
        in_specs=[vmem, vmem],
        out_specs=(hbm, hbm),
        scratch_shapes=[pltpu.SemaphoreType.DMA((2, parts))],
        compiler_params=pltpu.CompilerParams(vmem_limit_bytes=2**20),
        name="write_out",
    )(gate, up)
    return ready_gate, ready_up, fac[0, :cols], fac[0, cols:]


def solution(mesh):
    in_specs = (
        P("shard", "tp"),
        P("shard", None),
        P(None, "tp"),
        P("shard", "tp"),
        P("shard", None),
        P(None, "tp"),
        P("shard"),
    )
    out_specs = (P(None, "tp"), P(None, "tp"), P("tp"), P("tp"))
    n = mesh.shape[AXIS]
    side = math.isqrt(n // 2)
    body = functools.partial(paired, n) if side == 2 and 2 * side * side == n else local
    return jax.shard_map(body, mesh=mesh, in_specs=in_specs, out_specs=out_specs, check_vma=False)
```

```python
import functools
import math

import jax
import jax.numpy as jnp
from jax import lax
from jax.experimental import pallas as pl
from jax.experimental.pallas import tpu as pltpu
from jax.sharding import PartitionSpec as P

mix_rate = 2.0
AXIS = "shard"


def local(weight_gate, low_gate, high_gate, weight_up, low_up, high_up, norm_gain):
    latest_gate = weight_gate.astype(jnp.float32) + mix_rate * jnp.dot(
        low_gate, high_gate, preferred_element_type=jnp.float32
    )
    latest_up = weight_up.astype(jnp.float32) + mix_rate * jnp.dot(
        low_up, high_up, preferred_element_type=jnp.float32
    )
    latest_gained_gate = latest_gate * norm_gain[:, None]
    latest_gained_up = latest_up * norm_gain[:, None]
    total_gate, total_up = lax.psum(
        (
            jnp.sum(latest_gained_gate * latest_gained_gate, axis=0),
            jnp.sum(latest_gained_up * latest_gained_up, axis=0),
        ),
        AXIS,
    )
    factor_gate = jnp.sqrt(total_gate)
    factor_up = jnp.sqrt(total_up)
    narrow_gate = (latest_gained_gate / factor_gate).astype(jnp.bfloat16)
    narrow_up = (latest_gained_up / factor_up).astype(jnp.bfloat16)
    ready_gate = lax.all_gather(narrow_gate, AXIS, axis=0, tiled=True)
    ready_up = lax.all_gather(narrow_up, AXIS, axis=0, tiled=True)
    return (ready_gate, ready_up, factor_gate, factor_up)


def gather_kernel(
    n, chunks, raw, wg_hbm, wu_hbm, lg_hbm, lu_hbm, hg_hbm, hu_hbm, gain_hbm,
    out_g, out_u, fac,
    w_v, l_v, h_v, gain_v, low_v, g_v, col_v, sums, rf_v, far_low,
    in_sem, ssum, rsum, slow, rlow, send, recv,
):
    rows, cols = wg_hbm.shape
    step = rows // chunks
    me = lax.axis_index(AXIS)
    core = lax.rem(me, 2)
    x = lax.rem(me // 2, 2)
    y = me // 4
    sib = me + 1 - 2 * core
    to_x = me + 2 - 4 * x
    to_y = me + 4 - 8 * y
    diag = to_x + 4 - 8 * y

    barrier = pltpu.get_barrier_semaphore()
    for d in range(1, n):
        pl.semaphore_signal(barrier, inc=1, device_id={AXIS: lax.rem(me + d, n)})

    gain_load = pltpu.make_async_copy(gain_hbm, gain_v, in_sem.at[6])
    low_loads, high_loads, loads = (
        [
            pltpu.make_async_copy(src, dst.at[a], in_sem.at[3 * a + i])
            for a, src in enumerate(pair)
        ]
        for i, (pair, dst) in enumerate((
            ((lg_hbm, lu_hbm), l_v), ((hg_hbm, hu_hbm), h_v), ((wg_hbm, wu_hbm), w_v)
        ))
    )
    gain_load.start()
    for a in range(2):
        for c in (low_loads[a], high_loads[a], loads[a]):
            c.start()

    early = raw * step
    outs = (out_g, out_u)
    every = [(a, k) for a in range(2) for k in range(chunks)]
    started = {}

    def move(slot, a, k, owner, target, base=None):
        r = pl.ds(pl.multiple_of(owner * rows + k * step, 16), step)
        part = outs[a].at[r, :]
        return pltpu.make_async_remote_copy(
            src_ref=part if base is None else base.at[k * step:(k + 1) * step, :],
            dst_ref=part,
            send_sem=send.at[slot, a * chunks + k], recv_sem=recv.at[slot, a * chunks + k],
            device_id={AXIS: target})

    def go(*args):
        started[args[:3]] = move(*args)
        started[args[:3]].start()

    def send_own(a, k):
        go(0, a, k, me, to_x)
        go(1, a, k, me, to_y)
        go(2, a, k, me, sib)

    def send_raw(a, k):
        go(0, a, k, me, to_x, wg_hbm)
        go(1, a, k, me, to_y, wg_hbm)
        go(2, a, k, me, sib, wg_hbm)

    pl.semaphore_wait(barrier, n - 1)
    send_raw(0, 0)

    gain_load.wait()
    gain = gain_v[...].reshape(1, rows)
    col_v[...] = jnp.broadcast_to(gain, (128, rows)).T
    for a in range(2):
        low_loads[a].wait()
        low_v[a] = (mix_rate * l_v[a].astype(jnp.float32)).T.astype(jnp.bfloat16)
        high_loads[a].wait()
        loads[a].wait()
        acc = jnp.zeros((8, cols), jnp.float32)
        for k in range(chunks):
            r = pl.ds(k * step, step)
            prod = jnp.dot(low_v[a, r, :], h_v[a], preferred_element_type=jnp.float32)
            new = (w_v[a, r, :].astype(jnp.float32) + prod) * col_v[r, 0:1]
            g_v[a, r, :] = new
            acc = acc + jnp.sum((new * new).reshape(step // 8, 8, cols), axis=0)
        sums[me, :, a * cols:(a + 1) * cols] = jnp.sum(acc, axis=0, keepdims=True)

    sums[me, :, 2 * cols:] = gain[:, :early]
    shares = []
    for d in range(1, n):
        shares.append(pltpu.make_async_remote_copy(
            src_ref=sums.at[me], dst_ref=sums.at[me],
            send_sem=ssum.at[d], recv_sem=rsum.at[d],
            device_id={AXIS: lax.rem(me + d, n)}))
        shares[-1].start()
    lows = []
    for d in range(1, n):
        lows.append(pltpu.make_async_remote_copy(
            src_ref=l_v.at[0, :, :early], dst_ref=far_low.at[me],
            send_sem=slow.at[d], recv_sem=rlow.at[d],
            device_id={AXIS: lax.rem(me + d, n)}))
        lows[-1].start()
    for k in range(1, raw):
        send_raw(0, k)
    for c in shares:
        c.wait_recv()
    total = sums[0, :, :2 * cols]
    for d in range(1, n):
        total = total + sums[d, :, :2 * cols]
    factor = jnp.sqrt(total)
    fac[...] = factor
    rf_v[...] = 1.0 / factor

    for i, (a, k) in enumerate(every):
        new = g_v[a, k * step:(k + 1) * step, :] * rf_v[:, a * cols:(a + 1) * cols]
        r = pl.ds(pl.multiple_of(me * rows + k * step, 16), step)
        outs[a][r, :] = new.astype(jnp.bfloat16)
        if i > raw:
            send_own(*every[i - 1])
    send_own(*every[-1])

    for i, (a, k) in enumerate(every):
        move(0, a, k, to_x, to_x).wait_recv()
        if i % 2 == 0:
            go(5, a, k, to_x, to_y)
        go(3, a, k, to_x, sib)
        move(1, a, k, to_y, to_y).wait_recv()
        if i % 2 == 1:
            go(5, a, k, to_y, to_x)
        go(4, a, k, to_y, sib)

    flip = 1 - 2 * core

    def from_sib(a, k):
        move(2, a, k, sib, sib).wait_recv()
        move(3, a, k, to_x + flip, sib).wait_recv()
        move(4, a, k, to_y + flip, sib).wait_recv()
        move(6, a, k, diag + flip, sib).wait_recv()

    def finish_raw():
        for a, k in every[:raw]:
            from_sib(a, k)
            for slot in (3, 4, 5, 6):
                started.pop((slot, a, k)).wait_send()
        for c in lows:
            c.wait_recv()

        @pl.loop(1, n)
        def _(d):
            owner = lax.rem(me + d, n)
            low = (mix_rate * far_low[owner].astype(jnp.float32)).T.astype(jnp.bfloat16)
            col = jnp.broadcast_to(sums[owner, :, 2 * cols:], (128, early)).T[:, 0:1]
            r = pl.ds(pl.multiple_of(owner * rows, 16), early)
            prod = jnp.dot(low, h_v[0], preferred_element_type=jnp.float32)
            new = (out_g[r, :].astype(jnp.float32) + prod) * col
            out_g[r, :] = (new * rf_v[:, :cols]).astype(jnp.bfloat16)

    for i, (a, k) in enumerate(every):
        if i == 3 * raw:
            finish_raw()
        move(5, a, k, diag, to_x).wait_recv()
        go(6, a, k, diag, sib)
    for a, k in every[raw:]:
        from_sib(a, k)
    for c in started.values():
        c.wait_send()
    for c in shares + lows:
        c.wait_send()


def write_kernel(
    parts, a_v, b_v, fac, a_hbm, b_hbm, fa_hbm, fb_hbm, fac_v, fa_v, fb_v, sem, fsem
):
    step = a_v.shape[0] // parts
    cols = a_v.shape[1]
    load = pltpu.make_async_copy(fac, fac_v, fsem.at[0])
    load.start()
    copies = []
    for i, (src, dst) in enumerate(((a_v, a_hbm), (b_v, b_hbm))):
        for k in range(parts):
            r = pl.ds(k * step, step)
            copies.append(pltpu.make_async_copy(src.at[r, :], dst.at[r, :], sem.at[i, k]))
    for c in copies:
        c.start()
    load.wait()
    for i, (line, dst) in enumerate(((fa_v, fa_hbm), (fb_v, fb_hbm))):
        line[...] = fac_v[0, i * cols:(i + 1) * cols]
        copies.append(pltpu.make_async_copy(line, dst, fsem.at[1 + i]))
        copies[-1].start()
    for c in copies:
        c.wait()


def paired(n, weight_gate, low_gate, high_gate, weight_up, low_up, high_up, norm_gain):
    rows, cols = weight_gate.shape
    chunks, raw = 5, 2
    early = raw * rows // chunks
    full = (n * rows, cols)
    vmem = pl.BlockSpec(memory_space=pltpu.VMEM)
    hbm = pl.BlockSpec(memory_space=pl.ANY)
    gain = norm_gain
    space = pl.BlockSpec(memory_space=pltpu.HBM)
    rank = high_gate.shape[0]
    grant = 65472 * 2**10 - (4 * full[0] * cols + 8 * cols) // 2**10 * 2**10 - 24 * 2**10
    gate, up, fac = pl.pallas_call(
        functools.partial(gather_kernel, n, chunks, raw),
        out_shape=(
            pltpu.VMEM(full, jnp.bfloat16),
            pltpu.VMEM(full, jnp.bfloat16),
            jax.ShapeDtypeStruct((1, 2 * cols), jnp.float32),
        ),
        in_specs=[space] * 7,
        out_specs=(vmem, vmem, vmem),
        scratch_shapes=[
            pltpu.VMEM((2, rows, cols), jnp.bfloat16),
            pltpu.VMEM((2, rank, rows), jnp.bfloat16),
            pltpu.VMEM((2, rank, cols), jnp.bfloat16),
            pltpu.VMEM((rows,), jnp.float32),
            pltpu.VMEM((2, rows, rank), jnp.bfloat16),
            pltpu.VMEM((2, rows, cols), jnp.float32),
            pltpu.VMEM((rows, 128), jnp.float32),
            pltpu.VMEM((n, 1, 2 * cols + early), jnp.float32),
            pltpu.VMEM((1, 2 * cols), jnp.float32),
            pltpu.VMEM((n, rank, early), jnp.bfloat16),
            pltpu.SemaphoreType.DMA((7,)),
            pltpu.SemaphoreType.DMA((n,)),
            pltpu.SemaphoreType.DMA((n,)),
            pltpu.SemaphoreType.DMA((n,)),
            pltpu.SemaphoreType.DMA((n,)),
            pltpu.SemaphoreType.DMA((7, 2 * chunks)),
            pltpu.SemaphoreType.DMA((7, 2 * chunks)),
        ],
        compiler_params=pltpu.CompilerParams(
            collective_id=0, has_side_effects=True, vmem_limit_bytes=grant
        ),
        name="merge_gather",
    )(weight_gate, weight_up, low_gate.T, low_up.T, high_gate, high_up, gain)
    parts = 8
    return tuple(pl.pallas_call(
        functools.partial(write_kernel, parts),
        out_shape=(jax.ShapeDtypeStruct(full, jnp.bfloat16),) * 2
        + (jax.ShapeDtypeStruct((cols,), jnp.float32),) * 2,
        in_specs=[vmem, vmem, hbm],
        out_specs=(hbm,) * 4,
        scratch_shapes=[
            pltpu.VMEM((1, 2 * cols), jnp.float32),
            pltpu.VMEM((cols,), jnp.float32),
            pltpu.VMEM((cols,), jnp.float32),
            pltpu.SemaphoreType.DMA((2, parts)),
            pltpu.SemaphoreType.DMA((3,)),
        ],
        compiler_params=pltpu.CompilerParams(vmem_limit_bytes=grant),
        name="write_out",
    )(gate, up, fac))


def solution(mesh):
    in_specs = (
        P("shard", "tp"),
        P("shard", None),
        P(None, "tp"),
        P("shard", "tp"),
        P("shard", None),
        P(None, "tp"),
        P("shard"),
    )
    out_specs = (P(None, "tp"), P(None, "tp"), P("tp"), P("tp"))
    n = mesh.shape[AXIS]
    side = math.isqrt(n // 2)
    body = functools.partial(paired, n) if side == 2 and 2 * side * side == n else local
    return jax.shard_map(body, mesh=mesh, in_specs=in_specs, out_specs=out_specs, check_vma=False)
```
